16 devices in a mesh: rep: 2 (over y, z), dp: 8 (over x, core).
Axes of the slice: x: 4, y: 2, z: 1, core: 2. Of those that a mesh axis runs over, the one named last changes fastest.
The devices are a block of a 4x4x8 slice.
Arguments:
- x: bfloat16 [16, 2048, 1280], P(('rep', 'dp')), parts along dimension 0
- dy: bfloat16 [16, 2048, 1280], P(('rep', 'dp')), parts along dimension 0
- w_gate: bfloat16 [2, 1280, 4480], P(None, 'dp')
- w_up: bfloat16 [2, 1280, 4480], P(None, 'dp')
- w_down: bfloat16 [2, 4480, 1280], P(None, 'dp')
- m_w_gate: float32 [2, 1280, 4480], P(None, 'dp')
- m_w_up: float32 [2, 1280, 4480], P(None, 'dp')
- m_w_down: float32 [2, 4480, 1280], P(None, 'dp')
- v_w_gate: float32 [2, 1280, 4480], P(None, 'dp')
- v_w_up: float32 [2, 1280, 4480], P(None, 'dp')
- v_w_down: float32 [2, 4480, 1280], P(None, 'dp')
Outputs:
- output 1: bfloat16 [4, 1280, 4480], P('rep', 'dp'), parts along dimension 0
- output 2: bfloat16 [4, 1280, 4480], P('rep', 'dp'), parts along dimension 0
- output 3: bfloat16 [4, 4480, 1280], P('rep', 'dp'), parts along dimension 0
- output 4: float32 [4, 1280, 4480], P('rep', 'dp'), parts along dimension 0
- output 5: float32 [4, 1280, 4480], P('rep', 'dp'), parts along dimension 0
- output 6: float32 [4, 4480, 1280], P('rep', 'dp'), parts along dimension 0
- output 7: float32 [4, 1280, 4480], P('rep', 'dp'), parts along dimension 0
- output 8: float32 [4, 1280, 4480], P('rep', 'dp'), parts along dimension 0
- output 9: float32 [4, 4480, 1280], P('rep', 'dp'), parts along dimension 0
There are 2 independent parts. The reference program is written for one: setup_inputs(seed, part) draws one part's arguments, and reference() takes and returns one part's arrays. A program takes and returns all parts, laid end to end along the dimension named above; an argument that names none is the same for every part.
All inputs are finite; a program needn't handle non-finite values.
Results may differ from the reference program's by a relative error of at most 0.022.
Values are sent between devices in bfloat16 or wider.
A program may use at most 768 MiB of HBM per device.

```python
import jax
import jax.numpy as jnp
from jax import lax

SEQUENCES = 8
TOKENS = 2048
D = 1280
FF = 4480
LAYERS = 2
NAMES = ("w_gate", "w_up", "w_down")
SHAPES = {"w_gate": (LAYERS, D, FF), "w_up": (LAYERS, D, FF), "w_down": (LAYERS, FF, D)}


def bump(key, n, height):
    away = (jnp.arange(n, dtype=jnp.int32) - jax.random.randint(key, (), 0, n, jnp.int32)) % n
    return jnp.where(away < n // 8, height, 1.0)


def together(key, own, strength):
    shared = jax.random.normal(key, own.shape[1:], jnp.float32)
    return (own + strength * shared) * lax.rsqrt(1 + strength * strength)


def setup_inputs(seed: int = 0, part: int = 0) -> dict:
    kx, kdy, ka, kb, kz, kf, kh, kl, *keys = jax.random.split(jax.random.key(seed), 8 + 3 * len(NAMES))
    kx, kdy, ka, kb = (jax.random.fold_in(k, part) for k in (kx, kdy, ka, kb))
    kw, km, kv = (keys[i::3] for i in range(3))
    shape = (SEQUENCES, TOKENS, D)
    much_x, much_dy = jax.random.uniform(kz, (2,), jnp.float32, 0.0, 1.0)
    loud = 2.0 ** jax.random.uniform(jax.random.fold_in(kz, 1), (), jnp.float32, -1.0, 2.0)
    layers = 2.0 ** jax.random.uniform(kl, (LAYERS, 1, 1), jnp.float32, -1.0, 1.0)
    x = together(ka, jax.random.normal(kx, shape, jnp.float32), much_x) * bump(kf, D, 4.0)
    dy = together(kb, jax.random.normal(kdy, shape, jnp.float32), much_dy)
    drawn = {"x": x.astype(jnp.bfloat16), "dy": (loud * dy * (SEQUENCES * TOKENS) ** -0.5).astype(jnp.bfloat16)}
    for key, name in zip(kw, NAMES, strict=True):
        w = jax.random.normal(key, SHAPES[name], jnp.float32) * SHAPES[name][1] ** -0.5
        drawn[name] = (w * {"w_gate": 1.0, "w_up": bump(kh, FF, 4.0), "w_down": layers}[name]).astype(jnp.bfloat16)
    for key, name in zip(km, NAMES, strict=True):
        drawn[f"m_{name}"] = 0.1 * jax.random.normal(key, SHAPES[name], jnp.float32)
    for key, name in zip(kv, NAMES, strict=True):
        drawn[f"v_{name}"] = jax.random.uniform(key, SHAPES[name], jnp.float32, 0.005, 0.015)
    return drawn


def matmul(a, w):
    return jnp.dot(a, w, preferred_element_type=jnp.float32).astype(jnp.bfloat16)


def normed(h):
    wide = h.astype(jnp.float32)
    scale = lax.rsqrt(jnp.mean(wide**2, -1, keepdims=True) + 1e-6)
    return (wide * scale).astype(jnp.bfloat16)


def layer(h, w):
    a = normed(h)
    gate = jnp.dot(a, w["w_gate"], preferred_element_type=jnp.float32)
    up = jnp.dot(a, w["w_up"], preferred_element_type=jnp.float32)
    return h + matmul((jax.nn.silu(gate) * up).astype(jnp.bfloat16), w["w_down"])


def adamw(w, m, v, g):
    m = 0.9 * m + 0.1 * g
    v = 0.95 * v + 0.05 * g * g
    step = m * lax.rsqrt(v + 1e-8) + 0.1 * w
    return (w - 0.02 * step).astype(jnp.bfloat16), m, v


def clipped(gradients, sum_of_squares, count):
    factor = jnp.minimum(1.0, 0.5 * lax.rsqrt(sum_of_squares / count + 1e-30))
    return [g * factor for g in gradients]


def stack(weights, h):
    return lax.scan(lambda h, w: (layer(h, w), None), h, weights)[0]


def reference(x, dy, w_gate, w_up, w_down, m_w_gate, m_w_up, m_w_down, v_w_gate, v_w_up, v_w_down):
    weights = dict(zip(NAMES, (w_gate, w_up, w_down), strict=True))

    def take(so_far, sequence):
        h, by_y = sequence
        _, back = jax.vjp(lambda w: stack(w, h), weights)
        return jax.tree.map(lambda total, term: total + term.astype(jnp.float32), so_far, back(by_y)[0]), None

    none_yet = {name: jnp.zeros(w.shape, jnp.float32) for name, w in weights.items()}
    by_weights, _ = lax.scan(take, none_yet, (x, dy))
    gradients = [by_weights[name].astype(jnp.bfloat16).astype(jnp.float32) for name in NAMES]
    gradients = clipped(gradients, sum(jnp.sum(g * g) for g in gradients), sum(g.size for g in gradients))
    new = [
        adamw(w.astype(jnp.float32), m, v, g)
        for w, m, v, g in zip((w_gate, w_up, w_down), (m_w_gate, m_w_up, m_w_down), (v_w_gate, v_w_up, v_w_down), gradients, strict=True)
    ]
    return tuple(one[which] for which in range(3) for one in new)
```

```python
import functools

import jax
import jax.numpy as jnp
from jax import lax
from jax.experimental import pallas as pl
from jax.experimental.pallas import tpu as pltpu
from jax.sharding import PartitionSpec as P

BF = jnp.bfloat16
WIDE, DEEP = 640, 256


def dot(a, b, dims):
    return lax.dot_general(a, b, (dims, ((), ())), preferred_element_type=jnp.float32)


def adamw(w, m, v, g):
    m = 0.9 * m + 0.1 * g
    v = 0.95 * v + 0.05 * g * g
    step = m * lax.rsqrt(v + 1e-8) + 0.1 * w
    return (w - 0.02 * step).astype(BF), m, v


MESH = pl.DeviceIdType.MESH
SECOND, THIRD, FOURTH, READY = 1, 2, 3, 4


def pieces(rows):
    theirs = rows * 3 // 10 // 16 * 16
    return rows - theirs, theirs


def forward_kernel(n, wide, deep, x_hbm, wg_hbm, wu_hbm, wd_hbm, g_hbm, u_hbm, ht_hbm, at_hbm, h_hbm, fg_hbm, fu_hbm, fd_hbm,
                   h, a, hid, wgu, wd, g_out, u_out, t_out, a_t, recv, whole, local, sent, load_g, load_u, load_d, out_sem, io_sem):
    layers, ff = wg_hbm.shape[0], wg_hbm.shape[2]
    tokens, d = x_hbm.shape
    chips, half = n // 2, tokens // 2
    step = half // 4
    ups, downs = ff // wide, d // deep
    per = 2 * ups + downs
    units = layers * per
    rep, me = lax.axis_index("rep"), lax.axis_index("dp")
    chip, core = me // 2, me % 2
    parity = rep % 2
    way = 1 - 2 * core
    there = lambda k: ((chip + k * way + 2 * chips) % chips) * 2 + core
    ahead, behind, across = there(1), there(-1), there(2)
    beside = chip * 2 + 1 - core
    to_ahead, to_behind, to_beside = ((rep, i) for i in (ahead, behind, beside))
    to_pair = (rep + 1 - 2 * parity, me)

    barrier = pltpu.get_barrier_semaphore()
    for device in (to_ahead, to_behind, to_beside, to_pair):
        pl.semaphore_signal(barrier, inc=1, device_id=device, device_id_type=MESH)
    pl.semaphore_wait(barrier, 4)

    def unit_views(kind, layer, chunk):
        block, whole_ref, width = ((wg_hbm, fg_hbm, wide), (wu_hbm, fu_hbm, wide), (wd_hbm, fd_hbm, deep))[kind]
        columns = pl.ds(pl.multiple_of(chunk * width, width), width)
        rows = block.shape[1]
        own = lambda start, size: block.at[layer, pl.ds(pl.multiple_of(start, 16), size), columns]
        full = lambda start, size: whole_ref.at[layer, pl.ds(pl.multiple_of(start, 16), size), columns]
        return rows, own, full

    def for_unit(t, body):
        layer, r = t // per, t % per
        ok = jnp.logical_and(t >= 0, t < units)
        for kind in range(3):
            here = r >= 2 * ups if kind == 2 else jnp.logical_and(r < 2 * ups, r % 2 == kind)

            @pl.when(jnp.logical_and(ok, here))
            def _():
                body(kind, t, layer, r - 2 * ups if kind == 2 else r // 2)

    def send(unit, src, dst, device, sem):
        pltpu.make_async_remote_copy(src_ref=src, dst_ref=dst, send_sem=sent.at[unit], recv_sem=sem, device_id=device, device_id_type=MESH).start()

    def arrived(ref, sem):
        pltpu.make_async_copy(ref, ref, sem).wait()

    def stage_one(kind, unit, layer, chunk):
        rows, own, full = unit_views(kind, layer, chunk)
        mine, theirs = pieces(rows)
        start = parity * theirs
        send(unit, own(start, mine), full(me * rows + start, mine), to_ahead, recv.at[unit, 0])
        send(unit, own(start, mine), full(me * rows + start, mine), to_behind, recv.at[unit, 1])
        send(unit, own(0, rows), full(me * rows, rows), to_beside, whole.at[unit])
        pltpu.make_async_copy(own(0, rows), full(me * rows, rows), local.at[unit]).start()

    def onward(unit, rows, full, block, pair_sem):
        mine, theirs = pieces(rows)
        start, give = block * rows + parity * theirs, block * rows + parity * mine
        send(unit, full(give, theirs), full(give, theirs), to_pair, pair_sem)
        send(unit, full(start, mine), full(start, mine), to_beside, whole.at[unit])

    def from_pair(unit, rows, full, block, sem):
        mine, theirs = pieces(rows)
        ref = full(block * rows + (1 - parity) * mine, theirs)
        arrived(ref, sem)
        send(unit, ref, ref, to_beside, whole.at[unit])

    def stage_two(kind, unit, layer, chunk):
        rows, _, full = unit_views(kind, layer, chunk)
        mine, theirs = pieces(rows)
        first = full(behind * rows + parity * theirs, mine)
        arrived(first, recv.at[unit, 0])
        send(unit, first, first, to_ahead, recv.at[unit, 2])
        onward(unit, rows, full, behind, recv.at[unit, 3])
        arrived(full(ahead * rows + parity * theirs, mine), recv.at[unit, 1])
        onward(unit, rows, full, ahead, recv.at[unit, 4])

    def stage_three(kind, unit, layer, chunk):
        rows, _, full = unit_views(kind, layer, chunk)
        mine, theirs = pieces(rows)
        arrived(full(across * rows + parity * theirs, mine), recv.at[unit, 2])
        onward(unit, rows, full, across, recv.at[unit, 5])
        from_pair(unit, rows, full, behind, recv.at[unit, 3])
        from_pair(unit, rows, full, ahead, recv.at[unit, 4])

    def stage_four(kind, unit, layer, chunk):
        rows, _, full = unit_views(kind, layer, chunk)
        from_pair(unit, rows, full, across, recv.at[unit, 5])

    def ready(kind, unit, layer, chunk):
        rows, own, full = unit_views(kind, layer, chunk)
        arrived(full(0, chips * rows), whole.at[unit])
        arrived(own(0, rows), local.at[unit])
        slot = chunk % 2
        if kind == 0:
            pltpu.make_async_copy(full(0, d), wgu.at[slot, :, pl.ds(0, wide)], load_g.at[slot]).start()
        elif kind == 1:
            pltpu.make_async_copy(full(0, d), wgu.at[slot, :, pl.ds(wide, wide)], load_u.at[slot]).start()
        else:

            @pl.when(layer + 1 < layers)
            def _():
                pltpu.make_async_copy(full(0, ff), wd.at[slot], load_d.at[slot]).start()

    def all_sent(kind, unit, layer, chunk):
        rows, _, full = unit_views(kind, layer, chunk)
        arrived(full(0, (n - 1) * rows), sent.at[unit])

    def norm():
        def some(i, _):
            at = pl.ds(pl.multiple_of(i * 256, 256), 256)
            w = h[at, :].astype(jnp.float32)
            some_a = (w * lax.rsqrt(jnp.mean(w * w, -1, keepdims=True) + 1e-6)).astype(BF)
            a[at, :] = some_a
            a_t[:, at] = some_a.T
            return 0

        lax.fori_loop(0, tokens // 256, some, 0)

    def results(layer, chunk, part):
        at = pl.ds(pl.multiple_of(part * half, half), half)
        columns = pl.ds(pl.multiple_of(chunk * wide, wide), wide)
        return (
            pltpu.make_async_copy(g_out.at[part], g_hbm.at[layer, at, columns], out_sem.at[part, 0]),
            pltpu.make_async_copy(u_out.at[part], u_hbm.at[layer, at, columns], out_sem.at[part, 1]),
            pltpu.make_async_copy(t_out.at[part], ht_hbm.at[layer, columns, at], out_sem.at[part, 2]),
        )

    def gate_up(layer, chunk, part):
        slot = chunk % 2

        @pl.when(part == 0)
        def _():
            arrived(wgu.at[slot, :, pl.ds(0, wide)], load_g.at[slot])
            arrived(wgu.at[slot, :, pl.ds(wide, wide)], load_u.at[slot])

        @pl.when(jnp.logical_or(layer > 0, chunk > 0))
        def _():
            for copy in results(layer, chunk, part):
                copy.wait()

        def some(i, _):
            at = pl.ds(pl.multiple_of(part * half + i * step, step), step)
            out = pl.ds(pl.multiple_of(i * step, step), step)
            rows = a[at, :]
            both = jnp.dot(rows, wgu[slot], preferred_element_type=jnp.float32)
            gate, up = both[:, :wide], both[:, wide:]
            g_out[part, out, :] = gate
            u_out[part, out, :] = up
            on = (gate * jax.nn.sigmoid(gate) * up).astype(BF)
            hid[at, pl.ds(pl.multiple_of(chunk * wide, wide), wide)] = on
            t_out[part, :, out] = on.T
            return 0

        lax.fori_loop(0, half // step, some, 0)
        for copy in results(layer, chunk, part):
            copy.start()

    def down(layer, chunk):
        slot = chunk % 2
        arrived(wd.at[slot], load_d.at[slot])
        columns = pl.ds(pl.multiple_of(chunk * deep, deep), deep)

        def some(i, _):
            at = pl.ds(pl.multiple_of(i * step, step), step)
            y = jnp.dot(hid[at, :], wd[slot], preferred_element_type=jnp.float32).astype(BF)
            h[at, columns] = h[at, columns] + y
            return 0

        lax.fori_loop(0, tokens // step, some, 0)

    def states(layer):
        return (
            pltpu.make_async_copy(h, h_hbm.at[layer], io_sem.at[0]),
            pltpu.make_async_copy(a_t, at_hbm.at[layer], io_sem.at[1]),
        )

    def comm(t):
        for_unit(t, stage_one)
        for_unit(t - SECOND, stage_two)
        for_unit(t - THIRD, stage_three)
        for_unit(t - FOURTH, stage_four)
        for_unit(t - READY, ready)

    fetch = pltpu.make_async_copy(x_hbm, h, io_sem.at[0])
    fetch.start()
    fetch.wait()
    norm()
    for copy in states(0):
        copy.start()

    def tick(t, _):
        comm(t)
        u = t - READY - 1
        layer, r = u // per, u % per
        ok = jnp.logical_and(u >= 0, u < units)

        @pl.when(jnp.logical_and(ok, jnp.logical_and(r >= 1, r <= 2 * ups)))
        def _():
            gate_up(layer, (r - 1) // 2, (r - 1) % 2)

        @pl.when(jnp.logical_and(ok, jnp.logical_and(layer + 1 < layers, r >= 2 * ups)))
        def _():
            @pl.when(r == 2 * ups)
            def _():
                for copy in states(layer):
                    copy.wait()

            down(layer, r - 2 * ups)

            @pl.when(r == per - 1)
            def _():
                norm()
                for copy in states(layer + 1):
                    copy.start()

        return 0

    lax.fori_loop(0, units + READY + 1, tick, 0)
    for copy in (*results(layers - 1, ups - 1, 0), *results(layers - 1, ups - 1, 1), *states(layers - 1)):
        copy.wait()

    def finish(t, _):
        for_unit(t, all_sent)
        return 0

    lax.fori_loop(0, units, finish, 0)


def forward(x, w_gate, w_up, w_down, n):
    layers, _, ff = w_gate.shape
    tokens, d = x.shape
    wide, deep = WIDE, DEEP
    units = layers * (2 * (ff // wide) + d // deep)
    half = tokens // 2
    any_space = pl.BlockSpec(memory_space=pl.ANY)
    shape = jax.ShapeDtypeStruct
    out_shape = (
        shape((layers, tokens, ff), jnp.float32),
        shape((layers, tokens, ff), jnp.float32),
        shape((layers, ff, tokens), BF),
        shape((layers, d, tokens), BF),
        shape((layers, tokens, d), BF),
        shape((layers, d, ff), BF),
        shape((layers, d, ff), BF),
        shape((layers, ff, d), BF),
    )
    return pl.pallas_call(
        functools.partial(forward_kernel, n, wide, deep),
        out_shape=out_shape,
        in_specs=[any_space] * 4,
        out_specs=[any_space] * len(out_shape),
        scratch_shapes=[
            pltpu.VMEM((tokens, d), BF),
            pltpu.VMEM((tokens, d), BF),
            pltpu.VMEM((tokens, ff), BF),
            pltpu.VMEM((2, d, 2 * wide), BF),
            pltpu.VMEM((2, ff, deep), BF),
            pltpu.VMEM((2, half, wide), jnp.float32),
            pltpu.VMEM((2, half, wide), jnp.float32),
            pltpu.VMEM((2, wide, half), BF),
            pltpu.VMEM((d, tokens), BF),
            pltpu.SemaphoreType.DMA((units, 6)),
            pltpu.SemaphoreType.DMA((units,)),
            pltpu.SemaphoreType.DMA((units,)),
            pltpu.SemaphoreType.DMA((units,)),
            pltpu.SemaphoreType.DMA((2,)),
            pltpu.SemaphoreType.DMA((2,)),
            pltpu.SemaphoreType.DMA((2,)),
            pltpu.SemaphoreType.DMA((2, 3)),
            pltpu.SemaphoreType.DMA((2,)),
        ],
        compiler_params=pltpu.CompilerParams(collective_id=0, has_side_effects=True, vmem_limit_bytes=62 * 2**20),
        cost_estimate=pl.CostEstimate(flops=10 * tokens * d * ff, bytes_accessed=4 * layers * tokens * ff * 4, transcendentals=0),
    )(x, w_gate, w_up, w_down)


SUM_CHIP, SUM_NEAR, SUM_ALL = 1, 3, 5
HELD, FAR, NEAR = SUM_ALL + 1, SUM_NEAR - SUM_CHIP + 1, SUM_ALL - SUM_NEAR + 1


def backward_kernel(n, dy_hbm, h_hbm, at_hbm, ht_hbm, g_hbm, u_hbm, wg_hbm, wu_hbm, wd_hbm, gg_hbm, gu_hbm, gd_hbm, factor_out,
                    left, right, da, wd, wgu, gin, uin, hin, acc, sb, rb, sf, rh, sn, rn, so, sq, sqs,
                    left_sem, wd_sem, wgu_sem, gin_sem, hin_sem, out_sem, sb_sem, rb_sem, sf_sem, rh_sem, sn_sem, rn_sem,
                    free_b, free_h, free_n, sq_sem):
    layers, ff = g_hbm.shape[0], g_hbm.shape[2]
    tokens, d = dy_hbm.shape
    chips = n // 2
    part, wide = so.shape[1] // 2, so.shape[2]
    chunks, downs = ff // wide, ff // n // part
    splits = d // n // part
    per = downs + chunks * splits
    units = layers * per
    rep, me = lax.axis_index("rep"), lax.axis_index("dp")
    chip, core = me // 2, me % 2
    device = lambda c, k: (rep, (c % chips) * 2 + k)
    ahead, behind, beside = device(chip + 1, core), device(chip + chips - 1, core), device(chip, 1 - core)
    rows = 256

    barrier = pltpu.get_barrier_semaphore()

    def greet(i, _):
        pl.semaphore_signal(barrier, inc=1, device_id=(rep, (me + i) % n), device_id_type=MESH)
        return 0

    lax.fori_loop(1, n, greet, 0)
    pl.semaphore_wait(barrier, n - 1)

    def arrived(ref, sem):
        pltpu.make_async_copy(ref, ref, sem).wait()

    def send(src, dst, send_sem, recv_sem, to):
        pltpu.make_async_remote_copy(src_ref=src, dst_ref=dst, send_sem=send_sem, recv_sem=recv_sem, device_id=to, device_id_type=MESH).start()

    def signal(sem, to):
        pl.semaphore_signal(sem, inc=1, device_id=to, device_id_type=MESH)

    def place(u):
        return layers - 1 - u // per, u % per

    def load_left(src, layer, block, start, slot):
        for e in range(2):
            for q in range(chips):
                j = ((chip + q) % chips) * 2 + (core if e == 0 else 1 - core)
                at = pl.ds(pl.multiple_of(j * block + start, 16), part)
                pltpu.make_async_copy(src.at[layer, at, :], left.at[slot, pl.ds((e * chips + q) * part, part), :], left_sem.at[slot]).start()

    def left_ready(slot):
        arrived(left.at[slot], left_sem.at[slot])

    def chunk_columns(chunk):
        return pl.ds(pl.multiple_of(chunk * wide, wide), wide)

    def load_wd(layer, chunk):
        return pltpu.make_async_copy(wd_hbm.at[layer, chunk_columns(chunk), :], wd, wd_sem)

    def load_wgu(layer, chunk):
        return (
            pltpu.make_async_copy(wg_hbm.at[layer, :, chunk_columns(chunk)], wgu.at[:, pl.ds(0, wide)], wgu_sem.at[0]),
            pltpu.make_async_copy(wu_hbm.at[layer, :, chunk_columns(chunk)], wgu.at[:, pl.ds(wide, wide)], wgu_sem.at[1]),
        )

    def load_gate_up(layer, chunk, i):
        at = pl.ds(pl.multiple_of(i * rows, rows), rows)
        slot = i % 2
        return (
            pltpu.make_async_copy(g_hbm.at[layer, at, chunk_columns(chunk)], gin.at[slot], gin_sem.at[slot, 0]),
            pltpu.make_async_copy(u_hbm.at[layer, at, chunk_columns(chunk)], uin.at[slot], gin_sem.at[slot, 1]),
        )

    def load_h(layer, i):
        return pltpu.make_async_copy(h_hbm.at[layer, pl.ds(pl.multiple_of(i * rows, rows), rows), :], hin.at[i % 2], hin_sem.at[i % 2])

    def by_hidden(layer, chunk):
        load_wd(layer, chunk).wait()

        def some(i, _):
            at = pl.ds(pl.multiple_of(i * rows, rows), rows)
            slot = i % 2
            for copy in load_gate_up(layer, chunk, i):
                copy.wait()
            by = dot(right[0, at, :], wd[...], ((1,), (1,))).astype(BF).astype(jnp.float32)
            gate, up = gin[slot], uin[slot]
            on = jax.nn.sigmoid(gate)
            right[1, at, pl.ds(0, wide)] = (by * up * (on + gate * on * (1.0 - on))).astype(BF)
            right[1, at, pl.ds(wide, wide)] = (by * (gate * on)).astype(BF)

            @pl.when(i + 2 < tokens // rows)
            def _():
                for copy in load_gate_up(layer, chunk, i + 2):
                    copy.start()

            return 0

        lax.fori_loop(0, tokens // rows, some, 0)

    def by_normed(chunk):
        def some(i, _):
            at = pl.ds(pl.multiple_of(i * rows, rows), rows)
            by = dot(right[1, at, :], wgu[...], ((1,), (1,)))
            da[at, :] = jnp.where(chunk == 0, 0.0, da[at, :]) + by
            return 0

        lax.fori_loop(0, tokens // rows, some, 0)

    def by_states(layer):
        def some(i, _):
            at = pl.ds(pl.multiple_of(i * rows, rows), rows)
            load_h(layer, i).wait()
            w = hin[i % 2].astype(jnp.float32)
            by = da[at, :].astype(BF).astype(jnp.float32)
            scale = lax.rsqrt(jnp.mean(w * w, -1, keepdims=True) + 1e-6)
            back = by * scale - w * (scale * scale * scale * jnp.mean(by * w, -1, keepdims=True))
            right[0, at, :] = right[0, at, :] + back.astype(BF)

            @pl.when(i + 2 < tokens // rows)
            def _():
                load_h(layer, i + 2).start()

            return 0

        lax.fori_loop(0, tokens // rows, some, 0)

    def products(u, lefts, rights):
        two, held = u % 2, u % HELD

        @pl.when(u >= 2)
        def _():
            arrived(sb.at[two], sb_sem.at[two])

        def some(i, _):
            e = 1 - i
            lhs = left[lefts, pl.ds(pl.multiple_of(e * chips * part, 16), chips * part), :]
            by = dot(lhs, right[rights], ((1,), (0,)))
            for side in range(2):
                for q in range(chips):
                    block = by[q * part : (q + 1) * part, side * wide : (side + 1) * wide]

                    @pl.when(e == 1)
                    def _():
                        sb[two, q, side * part : (side + 1) * part, :] = block.astype(BF)

                    @pl.when(e == 0)
                    def _():
                        acc[held, q, side * part : (side + 1) * part, :] = block

            @pl.when(e == 1)
            def _():
                @pl.when(u >= 2)
                def _():
                    pl.semaphore_wait(free_b, 1)

                send(sb.at[two], rb.at[two], sb_sem.at[two], rb_sem.at[two], beside)

            return 0

        lax.fori_loop(0, 2, some, 0)

    first, second = pl.ds(0, part), pl.ds(part, part)

    def sum_chip(u):
        two, held, far = u % 2, u % HELD, u % FAR
        arrived(rb.at[two], rb_sem.at[two])

        @pl.when(u >= FAR)
        def _():
            arrived(sf.at[far, first], sf_sem.at[far, 0])
            arrived(sf.at[far, second], sf_sem.at[far, 1])

        sf[far] = (acc[held, 2] + rb[two, 2].astype(jnp.float32)).astype(BF)

        @pl.when(u >= FAR)
        def _():
            pl.semaphore_wait(free_h.at[0], 1)
            pl.semaphore_wait(free_h.at[1], 1)

        send(sf.at[far, first], rh.at[far, first], sf_sem.at[far, 0], rh_sem.at[far, 0], ahead)
        send(sf.at[far, second], rh.at[far, second], sf_sem.at[far, 1], rh_sem.at[far, 1], behind)
        for q in (1, 3, 0):
            acc[held, q] = acc[held, q] + rb[two, q].astype(jnp.float32)

        @pl.when(u < units - 2)
        def _():
            signal(free_b, beside)

    def sum_near(u):
        held, far, near = u % HELD, u % FAR, u % NEAR
        arrived(rh.at[far, first], rh_sem.at[far, 0])
        arrived(rh.at[far, second], rh_sem.at[far, 1])

        @pl.when(u >= NEAR)
        def _():
            arrived(sn.at[near, 0], sn_sem.at[near, 0])
            arrived(sn.at[near, 1], sn_sem.at[near, 1])

        sn[near, 0, first, :] = (acc[held, 1, first, :] + rh[far, first, :].astype(jnp.float32)).astype(BF)
        sn[near, 0, second, :] = acc[held, 1, second, :].astype(BF)
        sn[near, 1, first, :] = acc[held, 3, first, :].astype(BF)
        sn[near, 1, second, :] = (acc[held, 3, second, :] + rh[far, second, :].astype(jnp.float32)).astype(BF)

        @pl.when(u < units - FAR)
        def _():
            signal(free_h.at[0], behind)
            signal(free_h.at[1], ahead)

        @pl.when(u >= NEAR)
        def _():
            pl.semaphore_wait(free_n.at[0], 1)
            pl.semaphore_wait(free_n.at[1], 1)

        send(sn.at[near, 0], rn.at[near, 0], sn_sem.at[near, 0], rn_sem.at[near, 0], ahead)
        send(sn.at[near, 1], rn.at[near, 1], sn_sem.at[near, 1], rn_sem.at[near, 1], behind)

    def for_results(u, do):
        layer, r = place(u)
        two = u % 2

        @pl.when(r < downs)
        def _():
            at = pl.ds(pl.multiple_of(r * part, 16), part)
            do(pltpu.make_async_copy(so.at[two, first], gd_hbm.at[layer, at, pl.ds(0, wide)], out_sem.at[two, 0]))
            do(pltpu.make_async_copy(so.at[two, second], gd_hbm.at[layer, at, pl.ds(wide, wide)], out_sem.at[two, 1]))

        @pl.when(r >= downs)
        def _():
            chunk, z = (r - downs) // splits, (r - downs) % splits
            at = pl.ds(pl.multiple_of(z * part, 16), part)
            do(pltpu.make_async_copy(so.at[two, first], gg_hbm.at[layer, at, chunk_columns(chunk)], out_sem.at[two, 0]))
            do(pltpu.make_async_copy(so.at[two, second], gu_hbm.at[layer, at, chunk_columns(chunk)], out_sem.at[two, 1]))

    def sum_all(u):
        held, near, two = u % HELD, u % NEAR, u % 2
        arrived(rn.at[near, 0], rn_sem.at[near, 0])
        arrived(rn.at[near, 1], rn_sem.at[near, 1])

        @pl.when(u >= 2)
        def _():
            arrived(so.at[two, first], out_sem.at[two, 0])
            arrived(so.at[two, second], out_sem.at[two, 1])

        g = (acc[held, 0] + rn[near, 0].astype(jnp.float32) + rn[near, 1].astype(jnp.float32)).astype(BF)
        so[two] = g
        wide_g = g.astype(jnp.float32)
        sq[...] += jnp.sum((wide_g * wide_g).reshape(2 * part // 8, 8, wide), axis=0)

        @pl.when(u < units - NEAR)
        def _():
            signal(free_n.at[0], behind)
            signal(free_n.at[1], ahead)

        for_results(u, lambda copy: copy.start())

    def when_unit(u, body):
        @pl.when(jnp.logical_and(u >= 0, u < units))
        def _():
            body(u)

    def compute(u):
        layer, r = place(u)

        @pl.when(r == 0)
        def _():
            for z in range(splits):
                load_left(at_hbm, layer, d // n, z * part, 2 + z)
            load_wd(layer, 0).start()

        @pl.when(r + 1 < downs)
        def _():
            load_left(ht_hbm, layer, ff // n, (r + 1) * part, (r + 1) % 2)

        @pl.when(jnp.logical_and(u + 1 < units, r == per - 1))
        def _():
            load_left(ht_hbm, layer - 1, ff // n, 0, 0)

        after_down = r - downs
        chunk, z = after_down // splits, after_down % splits

        @pl.when(jnp.logical_and(after_down + 1 >= 0, jnp.logical_and((after_down + 1) % splits == 0, r + 1 < per)))
        def _():
            for i in range(2):
                for copy in load_gate_up(layer, (after_down + 1) // splits, i):
                    copy.start()

        @pl.when(r < downs)
        def _():
            left_ready(r % 2)

        @pl.when(jnp.logical_and(after_down >= 0, z == 0))
        def _():
            @pl.when(layer > 0)
            def _():
                for copy in load_wgu(layer, chunk):
                    copy.start()

            by_hidden(layer, chunk)

            @pl.when(chunk + 1 < chunks)
            def _():
                load_wd(layer, chunk + 1).start()

        for first_z in range(splits):

            @pl.when(after_down == first_z)
            def _():
                left_ready(2 + first_z)

        products(u, jnp.where(r < downs, r % 2, 2 + z), jnp.where(r < downs, 0, 1))

        @pl.when(jnp.logical_and(layer > 0, jnp.logical_and(after_down >= 0, z == splits - 1)))
        def _():
            @pl.when(r == per - 1)
            def _():
                load_h(layer, 0).start()
                load_h(layer, 1).start()

            for copy in load_wgu(layer, chunk):
                copy.wait()
            by_normed(chunk)

            @pl.when(r == per - 1)
            def _():
                by_states(layer)

    sq[...] = jnp.zeros_like(sq)
    fetch = pltpu.make_async_copy(dy_hbm, right.at[0], wd_sem)
    fetch.start()
    load_left(ht_hbm, layers - 1, ff // n, 0, 0)
    fetch.wait()

    def tick(t, _):
        when_unit(t - SUM_ALL, sum_all)
        when_unit(t - SUM_NEAR, sum_near)
        when_unit(t - SUM_CHIP, sum_chip)
        when_unit(t, compute)
        return 0

    lax.fori_loop(0, units + SUM_ALL, tick, 0)

    for two in range(2):
        arrived(so.at[two, first], out_sem.at[two, 0])
        arrived(so.at[two, second], out_sem.at[two, 1])
        arrived(sb.at[two], sb_sem.at[two])
    for far in range(FAR):
        arrived(sf.at[far, first], sf_sem.at[far, 0])
        arrived(sf.at[far, second], sf_sem.at[far, 1])
    for near in range(NEAR):
        arrived(sn.at[near, 0], sn_sem.at[near, 0])
        arrived(sn.at[near, 1], sn_sem.at[near, 1])

    some = sq[:, 0:128]
    for i in range(1, wide // 128):
        some = some + sq[:, i * 128 : (i + 1) * 128]
    sqs[me] = some

    def tell(i, _):
        send(sqs.at[me], sqs.at[me], sq_sem.at[0], sq_sem.at[1], (rep, (me + i) % n))
        return 0

    lax.fori_loop(1, n, tell, 0)
    others = sqs.at[pl.ds(0, n - 1)]
    arrived(others, sq_sem.at[1])
    arrived(others, sq_sem.at[0])
    total = sqs[0]
    for i in range(1, n):
        total = total + sqs[i]
    mean = jnp.sum(total, keepdims=True) / (3 * layers * d * ff)
    factor_out[...] = jnp.broadcast_to(jnp.minimum(1.0, 0.5 * lax.rsqrt(mean + 1e-30)), factor_out.shape)


def backward(dy, h, a_t, hid_t, gate, up, whole, n):
    layers, tokens, ff = gate.shape
    d = dy.shape[1]
    wide, part = WIDE, d // n // 2
    any_space = pl.BlockSpec(memory_space=pl.ANY)
    shape, vmem, dma = jax.ShapeDtypeStruct, pltpu.VMEM, pltpu.SemaphoreType.DMA
    block = (2 * part, wide)
    return pl.pallas_call(
        functools.partial(backward_kernel, n),
        out_shape=(
            shape((layers, d // n, ff), BF),
            shape((layers, d // n, ff), BF),
            shape((layers, ff // n, d), BF),
            shape((8, 128), jnp.float32),
        ),
        in_specs=[any_space] * 9,
        out_specs=[any_space] * 3 + [pl.BlockSpec(memory_space=pltpu.VMEM)],
        scratch_shapes=[
            vmem((4, n * part, tokens), BF),
            vmem((2, tokens, d), BF),
            vmem((tokens, d), jnp.float32),
            vmem((wide, d), BF),
            vmem((d, 2 * wide), BF),
            vmem((2, 256, wide), jnp.float32),
            vmem((2, 256, wide), jnp.float32),
            vmem((2, 256, d), BF),
            vmem((HELD, n // 2, *block), jnp.float32),
            vmem((2, n // 2, *block), BF),
            vmem((2, n // 2, *block), BF),
            vmem((FAR, *block), BF),
            vmem((FAR, *block), BF),
            vmem((NEAR, 2, *block), BF),
            vmem((NEAR, 2, *block), BF),
            vmem((2, *block), BF),
            vmem((8, wide), jnp.float32),
            vmem((n, 8, 128), jnp.float32),
            dma((4,)),
            dma(()),
            dma((2,)),
            dma((2, 2)),
            dma((2,)),
            dma((2, 2)),
            dma((2,)),
            dma((2,)),
            dma((FAR, 2)),
            dma((FAR, 2)),
            dma((NEAR, 2)),
            dma((NEAR, 2)),
            pltpu.SemaphoreType.REGULAR,
            pltpu.SemaphoreType.REGULAR((2,)),
            pltpu.SemaphoreType.REGULAR((2,)),
            dma((2,)),
        ],
        compiler_params=pltpu.CompilerParams(collective_id=1, has_side_effects=True, vmem_limit_bytes=63 * 2**20),
        cost_estimate=pl.CostEstimate(flops=20 * tokens * d * ff, bytes_accessed=4 * layers * tokens * ff * 4, transcendentals=0),
    )(dy, h, a_t, hid_t, gate, up, *whole)


def solution(mesh):
    n = mesh.shape["dp"]

    def step(x, dy, *arrays):
        weights, m, v = (arrays[i : i + 3] for i in (0, 3, 6))
        gate, up, hid_t, a_t, h, *whole = forward(x[0], *weights, n)
        *gradients, factor = backward(dy[0], h, a_t, hid_t, gate, up, whole, n)
        factor = factor[0, 0]
        new = [adamw(w.astype(jnp.float32), m, v, g.astype(jnp.float32) * factor) for w, m, v, g in zip(weights, m, v, gradients, strict=True)]
        return tuple(one[which] for which in range(3) for one in new)

    states, cut = P(("rep", "dp"), None, None), P(None, "dp", None)
    return jax.shard_map(
        step,
        mesh=mesh,
        in_specs=(states, states) + (cut,) * 9,
        out_specs=(P("rep", "dp", None),) * 9,
        check_vma=False,
    )
```

```python
import functools

import jax
import jax.numpy as jnp
from jax import lax
from jax.experimental import pallas as pl
from jax.experimental.pallas import tpu as pltpu
from jax.sharding import PartitionSpec as P

BF = jnp.bfloat16
WIDE, DEEP = 640, 256


def dot(a, b, dims):
    return lax.dot_general(a, b, (dims, ((), ())), preferred_element_type=jnp.float32)


def adamw(w, m, v, g):
    m = 0.9 * m + 0.1 * g
    v = 0.95 * v + 0.05 * g * g
    step = m * lax.rsqrt(v + 1e-8) + 0.1 * w
    return (w - 0.02 * step).astype(BF), m, v


MESH = pl.DeviceIdType.MESH
SECOND, THIRD, FOURTH, READY = 2, 4, 6, 7

PASSING = THIRD + 1


def pieces(rows):
    theirs = rows // 3 // 16 * 16
    return rows - theirs, theirs


def forward_kernel(n, wide, deep, x_hbm, wg_hbm, wu_hbm, wd_hbm, g_hbm, u_hbm, ht_hbm, at_hbm, h_hbm, fg_hbm, fu_hbm, fd_hbm,
                   h, a, hid, wgu, wd, g_out, u_out, t_out, a_t, pass_wide, pass_deep, recv, whole, local, sent, load_g, load_u, load_d, out_sem, io_sem, pass_sem):
    layers, ff = wg_hbm.shape[0], wg_hbm.shape[2]
    tokens, d = x_hbm.shape
    chips, half = n // 2, tokens // 2
    step = half // 2
    ups, downs = ff // wide, d // deep
    per = 2 * ups + downs
    units = layers * per
    rep, me = lax.axis_index("rep"), lax.axis_index("dp")
    chip, core = me // 2, me % 2
    parity = rep % 2
    way = 1 - 2 * core
    there = lambda k: ((chip + k * way + 2 * chips) % chips) * 2 + core
    ahead, behind, across = there(1), there(-1), there(2)
    beside = chip * 2 + 1 - core
    to_ahead, to_behind, to_beside = ((rep, i) for i in (ahead, behind, beside))
    to_pair = (rep + 1 - 2 * parity, me)

    barrier = pltpu.get_barrier_semaphore()
    for device in (to_ahead, to_behind, to_beside, to_pair):
        pl.semaphore_signal(barrier, inc=1, device_id=device, device_id_type=MESH)
    pl.semaphore_wait(barrier, 4)

    def unit_views(kind, layer, chunk):
        block, whole_ref, width = ((wg_hbm, fg_hbm, wide), (wu_hbm, fu_hbm, wide), (wd_hbm, fd_hbm, deep))[kind]
        columns = pl.ds(pl.multiple_of(chunk * width, width), width)
        rows = block.shape[1]
        own = lambda start, size: block.at[layer, pl.ds(pl.multiple_of(start, 16), size), columns]
        full = lambda start, size: whole_ref.at[layer, pl.ds(pl.multiple_of(start, 16), size), columns]
        return rows, own, full

    def for_unit(t, body):
        layer, r = t // per, t % per
        ok = jnp.logical_and(t >= 0, t < units)
        for kind in range(3):
            here = r >= 2 * ups if kind == 2 else jnp.logical_and(r < 2 * ups, r % 2 == kind)

            @pl.when(jnp.logical_and(ok, here))
            def _():
                body(kind, t, layer, r - 2 * ups if kind == 2 else r // 2)

    def send(unit, src, dst, device, sem):
        pltpu.make_async_remote_copy(src_ref=src, dst_ref=dst, send_sem=sent.at[unit], recv_sem=sem, device_id=device, device_id_type=MESH).start()

    def arrived(ref, sem):
        pltpu.make_async_copy(ref, ref, sem).wait()

    def stage_one(kind, unit, layer, chunk):
        rows, own, full = unit_views(kind, layer, chunk)
        mine, theirs = pieces(rows)
        start = parity * theirs
        send(unit, own(start, mine), full(me * rows + start, mine), to_ahead, recv.at[unit, 0])
        send(unit, own(start, mine), full(me * rows + start, mine), to_behind, recv.at[unit, 1])
        send(unit, own(0, rows), full(me * rows, rows), to_beside, whole.at[unit])
        bounce = (pass_deep if kind == 2 else pass_wide).at[unit % PASSING]
        pltpu.make_async_copy(own(0, rows), bounce, pass_sem.at[unit % PASSING]).start()

    def onward(unit, rows, full, block, pair_sem):
        mine, theirs = pieces(rows)
        start, give = block * rows + parity * theirs, block * rows + parity * mine
        send(unit, full(give, theirs), full(give, theirs), to_pair, pair_sem)
        send(unit, full(start, mine), full(start, mine), to_beside, whole.at[unit])

    def from_pair(unit, rows, full, block, sem):
        mine, theirs = pieces(rows)
        ref = full(block * rows + (1 - parity) * mine, theirs)
        arrived(ref, sem)
        send(unit, ref, ref, to_beside, whole.at[unit])

    def stage_two(kind, unit, layer, chunk):
        rows, _, full = unit_views(kind, layer, chunk)
        bounce = (pass_deep if kind == 2 else pass_wide).at[unit % PASSING]
        arrived(bounce, pass_sem.at[unit % PASSING])
        pltpu.make_async_copy(bounce, full(me * rows, rows), local.at[unit]).start()
        mine, theirs = pieces(rows)
        first = full(behind * rows + parity * theirs, mine)
        arrived(first, recv.at[unit, 0])
        send(unit, first, first, to_ahead, recv.at[unit, 2])
        onward(unit, rows, full, behind, recv.at[unit, 3])
        arrived(full(ahead * rows + parity * theirs, mine), recv.at[unit, 1])
        onward(unit, rows, full, ahead, recv.at[unit, 4])

    def stage_three(kind, unit, layer, chunk):
        rows, own, full = unit_views(kind, layer, chunk)
        mine, theirs = pieces(rows)
        arrived(own(0, rows), local.at[unit])
        arrived(full(across * rows + parity * theirs, mine), recv.at[unit, 2])
        onward(unit, rows, full, across, recv.at[unit, 5])
        from_pair(unit, rows, full, behind, recv.at[unit, 3])
        from_pair(unit, rows, full, ahead, recv.at[unit, 4])

    def stage_four(kind, unit, layer, chunk):
        rows, _, full = unit_views(kind, layer, chunk)
        from_pair(unit, rows, full, across, recv.at[unit, 5])

    def ready(kind, unit, layer, chunk):
        rows, _, full = unit_views(kind, layer, chunk)
        arrived(full(0, chips * rows), whole.at[unit])
        slot = chunk % 2
        if kind == 0:
            pltpu.make_async_copy(full(0, d), wgu.at[slot, :, pl.ds(0, wide)], load_g.at[slot]).start()
        elif kind == 1:
            pltpu.make_async_copy(full(0, d), wgu.at[slot, :, pl.ds(wide, wide)], load_u.at[slot]).start()
        else:

            @pl.when(layer + 1 < layers)
            def _():
                pltpu.make_async_copy(full(0, ff), wd.at[slot], load_d.at[slot]).start()

    def all_sent(kind, unit, layer, chunk):
        rows, _, full = unit_views(kind, layer, chunk)
        arrived(full(0, (n - 1) * rows), sent.at[unit])

    def norm():
        def some(i, _):
            at = pl.ds(pl.multiple_of(i * 256, 256), 256)
            w = h[at, :].astype(jnp.float32)
            some_a = (w * lax.rsqrt(jnp.mean(w * w, -1, keepdims=True) + 1e-6)).astype(BF)
            a[at, :] = some_a
            a_t[:, at] = some_a.T
            return 0

        lax.fori_loop(0, tokens // 256, some, 0)

    def results(layer, chunk, part):
        at = pl.ds(pl.multiple_of(part * half, half), half)
        columns = pl.ds(pl.multiple_of(chunk * wide, wide), wide)
        return (
            pltpu.make_async_copy(g_out.at[part], g_hbm.at[layer, at, columns], out_sem.at[part, 0]),
            pltpu.make_async_copy(u_out.at[part], u_hbm.at[layer, at, columns], out_sem.at[part, 1]),
            pltpu.make_async_copy(t_out.at[part], ht_hbm.at[layer, columns, at], out_sem.at[part, 2]),
        )

    def gate_up(layer, chunk, part):
        slot = chunk % 2

        @pl.when(part == 0)
        def _():
            arrived(wgu.at[slot, :, pl.ds(0, wide)], load_g.at[slot])
            arrived(wgu.at[slot, :, pl.ds(wide, wide)], load_u.at[slot])

        @pl.when(jnp.logical_or(layer > 0, chunk > 0))
        def _():
            for copy in results(layer, chunk, part):
                copy.wait()

        def some(i, _):
            at = pl.ds(pl.multiple_of(part * half + i * step, step), step)
            out = pl.ds(pl.multiple_of(i * step, step), step)
            rows = a[at, :]
            both = jnp.dot(rows, wgu[slot], preferred_element_type=jnp.float32)
            gate, up = both[:, :wide], both[:, wide:]
            g_out[part, out, :] = gate
            u_out[part, out, :] = up
            on = (gate * jax.nn.sigmoid(gate) * up).astype(BF)
            hid[at, pl.ds(pl.multiple_of(chunk * wide, wide), wide)] = on
            t_out[part, :, out] = on.T
            return 0

        lax.fori_loop(0, half // step, some, 0)
        for copy in results(layer, chunk, part):
            copy.start()

    def down(layer, chunk):
        slot = chunk % 2
        arrived(wd.at[slot], load_d.at[slot])
        columns = pl.ds(pl.multiple_of(chunk * deep, deep), deep)

        def some(i, _):
            at = pl.ds(pl.multiple_of(i * step, step), step)
            y = jnp.dot(hid[at, :], wd[slot], preferred_element_type=jnp.float32).astype(BF)
            h[at, columns] = h[at, columns] + y
            return 0

        lax.fori_loop(0, tokens // step, some, 0)

    def states(layer):
        return (
            pltpu.make_async_copy(h, h_hbm.at[layer], io_sem.at[0]),
            pltpu.make_async_copy(a_t, at_hbm.at[layer], io_sem.at[1]),
        )

    def comm(t):
        for_unit(t, stage_one)
        for_unit(t - SECOND, stage_two)
        for_unit(t - THIRD, stage_three)
        for_unit(t - FOURTH, stage_four)
        for_unit(t - READY, ready)

    fetch = pltpu.make_async_copy(x_hbm, h, io_sem.at[0])
    fetch.start()

    def tick(t, _):
        comm(t)

        @pl.when(t == SECOND)
        def _():
            fetch.wait()
            norm()
            for copy in states(0):
                copy.start()

        u = t - READY - 1
        layer, r = u // per, u % per
        ok = jnp.logical_and(u >= 0, u < units)

        @pl.when(jnp.logical_and(ok, jnp.logical_and(r >= 1, r <= 2 * ups)))
        def _():
            gate_up(layer, (r - 1) // 2, (r - 1) % 2)

        @pl.when(jnp.logical_and(ok, jnp.logical_and(layer + 1 < layers, r >= 2 * ups)))
        def _():
            @pl.when(r == 2 * ups)
            def _():
                for copy in states(layer):
                    copy.wait()

            down(layer, r - 2 * ups)

            @pl.when(r == per - 1)
            def _():
                norm()
                for copy in states(layer + 1):
                    copy.start()

        return 0

    lax.fori_loop(0, units + READY + 1, tick, 0)
    for copy in (*results(layers - 1, ups - 1, 0), *results(layers - 1, ups - 1, 1), *states(layers - 1)):
        copy.wait()

    def finish(t, _):
        for_unit(t, all_sent)
        return 0

    lax.fori_loop(0, units, finish, 0)


def forward(x, w_gate, w_up, w_down, n):
    layers, _, ff = w_gate.shape
    tokens, d = x.shape
    wide, deep = WIDE, DEEP
    units = layers * (2 * (ff // wide) + d // deep)
    half = tokens // 2
    any_space = pl.BlockSpec(memory_space=pl.ANY)
    shape = jax.ShapeDtypeStruct
    out_shape = (
        shape((layers, tokens, ff), jnp.float32),
        shape((layers, tokens, ff), jnp.float32),
        shape((layers, ff, tokens), BF),
        shape((layers, d, tokens), BF),
        shape((layers, tokens, d), BF),
        shape((layers, d, ff), BF),
        shape((layers, d, ff), BF),
        shape((layers, ff, d), BF),
    )
    return pl.pallas_call(
        functools.partial(forward_kernel, n, wide, deep),
        out_shape=out_shape,
        in_specs=[any_space] * 4,
        out_specs=[any_space] * len(out_shape),
        scratch_shapes=[
            pltpu.VMEM((tokens, d), BF),
            pltpu.VMEM((tokens, d), BF),
            pltpu.VMEM((tokens, ff), BF),
            pltpu.VMEM((2, d, 2 * wide), BF),
            pltpu.VMEM((2, ff, deep), BF),
            pltpu.VMEM((2, half, wide), jnp.float32),
            pltpu.VMEM((2, half, wide), jnp.float32),
            pltpu.VMEM((2, wide, half), BF),
            pltpu.VMEM((d, tokens), BF),
            pltpu.VMEM((PASSING, d // n, wide), BF),
            pltpu.VMEM((PASSING, ff // n, deep), BF),
            pltpu.SemaphoreType.DMA((units, 6)),
            pltpu.SemaphoreType.DMA((units,)),
            pltpu.SemaphoreType.DMA((units,)),
            pltpu.SemaphoreType.DMA((units,)),
            pltpu.SemaphoreType.DMA((2,)),
            pltpu.SemaphoreType.DMA((2,)),
            pltpu.SemaphoreType.DMA((2,)),
            pltpu.SemaphoreType.DMA((2, 3)),
            pltpu.SemaphoreType.DMA((2,)),
            pltpu.SemaphoreType.DMA((PASSING,)),
        ],
        compiler_params=pltpu.CompilerParams(collective_id=0, has_side_effects=True, vmem_limit_bytes=62 * 2**20),
        cost_estimate=pl.CostEstimate(flops=10 * tokens * d * ff, bytes_accessed=4 * layers * tokens * ff * 4, transcendentals=0),
    )(x, w_gate, w_up, w_down)


SUM_CHIP, SUM_NEAR, SUM_ALL = 1, 4, 7
FAR, NEAR = SUM_NEAR - SUM_CHIP + 1, SUM_ALL - SUM_NEAR + 1


def backward_kernel(n, dy_hbm, h_hbm, at_hbm, ht_hbm, g_hbm, u_hbm, wg_hbm, wu_hbm, wd_hbm, gg_hbm, gu_hbm, gd_hbm, factor_out,
                    left, right, da, wd, wgu, gin, uin, hin, acc_far, acc_near, acc_own, sb, rb, sf, rh, sn, rn, so, sq, sqs,
                    left_sem, wd_sem, wgu_sem, gin_sem, hin_sem, out_sem, sb_sem, rb_sem, sf_sem, rh_sem, sn_sem, rn_sem,
                    free_b, free_h, free_n, sq_sem):
    layers, ff = g_hbm.shape[0], g_hbm.shape[2]
    tokens, d = dy_hbm.shape
    chips = n // 2
    part, wide = so.shape[1] // 2, so.shape[2]
    chunks, downs = ff // wide, ff // n // part
    splits = d // n // part
    per = downs + chunks * splits
    units = layers * per
    rep, me = lax.axis_index("rep"), lax.axis_index("dp")
    chip, core = me // 2, me % 2
    device = lambda c, k: (rep, (c % chips) * 2 + k)
    ahead, behind, beside = device(chip + 1, core), device(chip + chips - 1, core), device(chip, 1 - core)
    rows, few = 512, 256

    barrier = pltpu.get_barrier_semaphore()

    def greet(i, _):
        pl.semaphore_signal(barrier, inc=1, device_id=(rep, (me + i) % n), device_id_type=MESH)
        return 0

    lax.fori_loop(1, n, greet, 0)
    pl.semaphore_wait(barrier, n - 1)

    def arrived(ref, sem):
        pltpu.make_async_copy(ref, ref, sem).wait()

    def send(src, dst, send_sem, recv_sem, to):
        pltpu.make_async_remote_copy(src_ref=src, dst_ref=dst, send_sem=send_sem, recv_sem=recv_sem, device_id=to, device_id_type=MESH).start()

    def signal(sem, to):
        pl.semaphore_signal(sem, inc=1, device_id=to, device_id_type=MESH)

    def place(u):
        return layers - 1 - u // per, u % per

    def load_left(src, layer, block, start, slot):
        for e in range(2):
            for q in range(chips):
                j = ((chip + q) % chips) * 2 + (core if e == 0 else 1 - core)
                at = pl.ds(pl.multiple_of(j * block + start, 16), part)
                pltpu.make_async_copy(src.at[layer, at, :], left.at[slot, pl.ds((e * chips + q) * part, part), :], left_sem.at[slot]).start()

    def left_ready(slot):
        arrived(left.at[slot], left_sem.at[slot])

    def chunk_columns(chunk):
        return pl.ds(pl.multiple_of(chunk * wide, wide), wide)

    def load_wd(layer, chunk):
        return pltpu.make_async_copy(wd_hbm.at[layer, chunk_columns(chunk), :], wd, wd_sem)

    def load_wgu(layer, chunk):
        return (
            pltpu.make_async_copy(wg_hbm.at[layer, :, chunk_columns(chunk)], wgu.at[:, pl.ds(0, wide)], wgu_sem.at[0]),
            pltpu.make_async_copy(wu_hbm.at[layer, :, chunk_columns(chunk)], wgu.at[:, pl.ds(wide, wide)], wgu_sem.at[1]),
        )

    def load_gate_up(layer, chunk, i):
        at = pl.ds(pl.multiple_of(i * rows, rows), rows)
        slot = i % 2
        return (
            pltpu.make_async_copy(g_hbm.at[layer, at, chunk_columns(chunk)], gin.at[slot], gin_sem.at[slot, 0]),
            pltpu.make_async_copy(u_hbm.at[layer, at, chunk_columns(chunk)], uin.at[slot], gin_sem.at[slot, 1]),
        )

    def load_h(layer, i):
        return pltpu.make_async_copy(h_hbm.at[layer, pl.ds(pl.multiple_of(i * few, few), few), :], hin.at[i % 2], hin_sem.at[i % 2])

    def by_hidden(layer, chunk):
        load_wd(layer, chunk).wait()

        def some(i, _):
            at = pl.ds(pl.multiple_of(i * rows, rows), rows)
            slot = i % 2
            for copy in load_gate_up(layer, chunk, i):
                copy.wait()
            by = dot(right[0, at, :], wd[...], ((1,), (1,))).astype(BF).astype(jnp.float32)
            gate, up = gin[slot], uin[slot]
            on = jax.nn.sigmoid(gate)
            right[1, at, pl.ds(0, wide)] = (by * up * (on + gate * on * (1.0 - on))).astype(BF)
            right[1, at, pl.ds(wide, wide)] = (by * (gate * on)).astype(BF)

            @pl.when(i + 2 < tokens // rows)
            def _():
                for copy in load_gate_up(layer, chunk, i + 2):
                    copy.start()

            return 0

        lax.fori_loop(0, tokens // rows, some, 0)

    def by_normed(chunk):
        def some(i, _):
            at = pl.ds(pl.multiple_of(i * rows, rows), rows)
            by = dot(right[1, at, :], wgu[...], ((1,), (1,)))
            da[at, :] = jnp.where(chunk == 0, 0.0, da[at, :]) + by
            return 0

        lax.fori_loop(0, tokens // rows, some, 0)

    def by_states(layer):
        def some(i, _):
            at = pl.ds(pl.multiple_of(i * few, few), few)
            load_h(layer, i).wait()
            w = hin[i % 2].astype(jnp.float32)
            by = da[at, :].astype(BF).astype(jnp.float32)
            scale = lax.rsqrt(jnp.mean(w * w, -1, keepdims=True) + 1e-6)
            back = by * scale - w * (scale * scale * scale * jnp.mean(by * w, -1, keepdims=True))
            right[0, at, :] = right[0, at, :] + back.astype(BF)

            @pl.when(i + 2 < tokens // few)
            def _():
                load_h(layer, i + 2).start()

            return 0

        lax.fori_loop(0, tokens // few, some, 0)

    def products(u, lefts, rights):
        two = u % 2

        @pl.when(u >= 2)
        def _():
            arrived(sb.at[two], sb_sem.at[two])

        by = dot(left[lefts], right[rights], ((1,), (0,)))
        for side in range(2):
            at, columns = pl.ds(side * part, part), slice(side * wide, (side + 1) * wide)
            block = lambda k: by[k * part : (k + 1) * part, columns]
            for q in range(chips):
                sb[two, q, at, :] = block(chips + q).astype(BF)
            acc_own[u % (SUM_ALL + 1), at, :] = block(0)
            acc_near[u % (SUM_NEAR + 1), 0, at, :] = block(1)
            acc_far[u % (SUM_CHIP + 1), at, :] = block(2)
            acc_near[u % (SUM_NEAR + 1), 1, at, :] = block(3)

        @pl.when(u >= 2)
        def _():
            pl.semaphore_wait(free_b, 1)

        send(sb.at[two], rb.at[two], sb_sem.at[two], rb_sem.at[two], beside)

    first, second = pl.ds(0, part), pl.ds(part, part)

    def sum_chip(u):
        two, far, nearby, own = u % 2, u % FAR, u % (SUM_NEAR + 1), u % (SUM_ALL + 1)
        arrived(rb.at[two], rb_sem.at[two])

        @pl.when(u >= FAR)
        def _():
            arrived(sf.at[far, first], sf_sem.at[far, 0])
            arrived(sf.at[far, second], sf_sem.at[far, 1])

        sf[far] = (acc_far[u % (SUM_CHIP + 1)] + rb[two, 2].astype(jnp.float32)).astype(BF)

        @pl.when(u >= FAR)
        def _():
            pl.semaphore_wait(free_h.at[0], 1)
            pl.semaphore_wait(free_h.at[1], 1)

        send(sf.at[far, first], rh.at[far, first], sf_sem.at[far, 0], rh_sem.at[far, 0], ahead)
        send(sf.at[far, second], rh.at[far, second], sf_sem.at[far, 1], rh_sem.at[far, 1], behind)
        for i in range(2):
            acc_near[nearby, i] = acc_near[nearby, i] + rb[two, 1 + 2 * i].astype(jnp.float32)
        acc_own[own] = acc_own[own] + rb[two, 0].astype(jnp.float32)

        @pl.when(u < units - 2)
        def _():
            signal(free_b, beside)

    def sum_near(u):
        held, far, near = u % (SUM_NEAR + 1), u % FAR, u % NEAR
        arrived(rh.at[far, first], rh_sem.at[far, 0])
        arrived(rh.at[far, second], rh_sem.at[far, 1])

        @pl.when(u >= NEAR)
        def _():
            arrived(sn.at[near, 0], sn_sem.at[near, 0])
            arrived(sn.at[near, 1], sn_sem.at[near, 1])

        sn[near, 0, first, :] = (acc_near[held, 0, first, :] + rh[far, first, :].astype(jnp.float32)).astype(BF)
        sn[near, 0, second, :] = acc_near[held, 0, second, :].astype(BF)
        sn[near, 1, first, :] = acc_near[held, 1, first, :].astype(BF)
        sn[near, 1, second, :] = (acc_near[held, 1, second, :] + rh[far, second, :].astype(jnp.float32)).astype(BF)

        @pl.when(u < units - FAR)
        def _():
            signal(free_h.at[0], behind)
            signal(free_h.at[1], ahead)

        @pl.when(u >= NEAR)
        def _():
            pl.semaphore_wait(free_n.at[0], 1)
            pl.semaphore_wait(free_n.at[1], 1)

        send(sn.at[near, 0], rn.at[near, 0], sn_sem.at[near, 0], rn_sem.at[near, 0], ahead)
        send(sn.at[near, 1], rn.at[near, 1], sn_sem.at[near, 1], rn_sem.at[near, 1], behind)

    def for_results(u, do):
        layer, r = place(u)
        two = u % 2

        @pl.when(r < downs)
        def _():
            at = pl.ds(pl.multiple_of(r * part, 16), part)
            do(pltpu.make_async_copy(so.at[two, first], gd_hbm.at[layer, at, pl.ds(0, wide)], out_sem.at[two, 0]))
            do(pltpu.make_async_copy(so.at[two, second], gd_hbm.at[layer, at, pl.ds(wide, wide)], out_sem.at[two, 1]))

        @pl.when(r >= downs)
        def _():
            chunk, z = (r - downs) // splits, (r - downs) % splits
            at = pl.ds(pl.multiple_of(z * part, 16), part)
            do(pltpu.make_async_copy(so.at[two, first], gg_hbm.at[layer, at, chunk_columns(chunk)], out_sem.at[two, 0]))
            do(pltpu.make_async_copy(so.at[two, second], gu_hbm.at[layer, at, chunk_columns(chunk)], out_sem.at[two, 1]))

    def sum_all(u):
        near, two = u % NEAR, u % 2
        arrived(rn.at[near, 0], rn_sem.at[near, 0])
        arrived(rn.at[near, 1], rn_sem.at[near, 1])

        @pl.when(u >= 2)
        def _():
            arrived(so.at[two, first], out_sem.at[two, 0])
            arrived(so.at[two, second], out_sem.at[two, 1])

        g = (acc_own[u % (SUM_ALL + 1)] + rn[near, 0].astype(jnp.float32) + rn[near, 1].astype(jnp.float32)).astype(BF)
        so[two] = g
        wide_g = g.astype(jnp.float32)
        sq[...] += jnp.sum((wide_g * wide_g).reshape(2 * part // 8, 8, wide), axis=0)

        @pl.when(u < units - NEAR)
        def _():
            signal(free_n.at[0], behind)
            signal(free_n.at[1], ahead)

        for_results(u, lambda copy: copy.start())

    def when_unit(u, body):
        @pl.when(jnp.logical_and(u >= 0, u < units))
        def _():
            body(u)

    def compute(u):
        layer, r = place(u)

        @pl.when(r == 0)
        def _():
            for z in range(splits):
                load_left(at_hbm, layer, d // n, z * part, 2 + z)
            load_wd(layer, 0).start()

        @pl.when(r + 1 < downs)
        def _():
            load_left(ht_hbm, layer, ff // n, (r + 1) * part, (r + 1) % 2)

        @pl.when(jnp.logical_and(u + 1 < units, r == per - 1))
        def _():
            load_left(ht_hbm, layer - 1, ff // n, 0, 0)

        after_down = r - downs
        chunk, z = after_down // splits, after_down % splits

        @pl.when(jnp.logical_and(after_down + 1 >= 0, jnp.logical_and((after_down + 1) % splits == 0, r + 1 < per)))
        def _():
            for i in range(2):
                for copy in load_gate_up(layer, (after_down + 1) // splits, i):
                    copy.start()

        @pl.when(r < downs)
        def _():
            left_ready(r % 2)

        @pl.when(jnp.logical_and(after_down >= 0, z == 0))
        def _():
            @pl.when(layer > 0)
            def _():
                for copy in load_wgu(layer, chunk):
                    copy.start()

            by_hidden(layer, chunk)

            @pl.when(chunk + 1 < chunks)
            def _():
                load_wd(layer, chunk + 1).start()

        for first_z in range(splits):

            @pl.when(after_down == first_z)
            def _():
                left_ready(2 + first_z)

        products(u, jnp.where(r < downs, r % 2, 2 + z), jnp.where(r < downs, 0, 1))

        @pl.when(jnp.logical_and(layer > 0, jnp.logical_and(after_down >= 0, z == splits - 1)))
        def _():
            @pl.when(r == per - 1)
            def _():
                load_h(layer, 0).start()
                load_h(layer, 1).start()

            for copy in load_wgu(layer, chunk):
                copy.wait()
            by_normed(chunk)

            @pl.when(r == per - 1)
            def _():
                by_states(layer)

    sq[...] = jnp.zeros_like(sq)
    fetch = pltpu.make_async_copy(dy_hbm, right.at[0], wd_sem)
    fetch.start()
    load_left(ht_hbm, layers - 1, ff // n, 0, 0)
    fetch.wait()

    def tick(t, _):
        when_unit(t - SUM_ALL, sum_all)
        when_unit(t - SUM_NEAR, sum_near)
        when_unit(t, compute)
        when_unit(t - SUM_CHIP, sum_chip)
        return 0

    lax.fori_loop(0, units + SUM_ALL, tick, 0)

    for two in range(2):
        arrived(so.at[two, first], out_sem.at[two, 0])
        arrived(so.at[two, second], out_sem.at[two, 1])
        arrived(sb.at[two], sb_sem.at[two])
    for far in range(FAR):
        arrived(sf.at[far, first], sf_sem.at[far, 0])
        arrived(sf.at[far, second], sf_sem.at[far, 1])
    for near in range(NEAR):
        arrived(sn.at[near, 0], sn_sem.at[near, 0])
        arrived(sn.at[near, 1], sn_sem.at[near, 1])

    some = sq[:, 0:128]
    for i in range(1, wide // 128):
        some = some + sq[:, i * 128 : (i + 1) * 128]
    sqs[me] = some

    def tell(i, _):
        send(sqs.at[me], sqs.at[me], sq_sem.at[0], sq_sem.at[1], (rep, (me + i) % n))
        return 0

    lax.fori_loop(1, n, tell, 0)
    others = sqs.at[pl.ds(0, n - 1)]
    arrived(others, sq_sem.at[1])
    arrived(others, sq_sem.at[0])
    total = sqs[0]
    for i in range(1, n):
        total = total + sqs[i]
    mean = jnp.sum(total, keepdims=True) / (3 * layers * d * ff)
    factor_out[...] = jnp.broadcast_to(jnp.minimum(1.0, 0.5 * lax.rsqrt(mean + 1e-30)), factor_out.shape)


def backward(dy, h, a_t, hid_t, gate, up, whole, n):
    layers, tokens, ff = gate.shape
    d = dy.shape[1]
    wide, part = WIDE, d // n // 2
    any_space = pl.BlockSpec(memory_space=pl.ANY)
    shape, vmem, dma = jax.ShapeDtypeStruct, pltpu.VMEM, pltpu.SemaphoreType.DMA
    block = (2 * part, wide)
    return pl.pallas_call(
        functools.partial(backward_kernel, n),
        out_shape=(
            shape((layers, d // n, ff), BF),
            shape((layers, d // n, ff), BF),
            shape((layers, ff // n, d), BF),
            shape((8, 128), jnp.float32),
        ),
        in_specs=[any_space] * 9,
        out_specs=[any_space] * 3 + [pl.BlockSpec(memory_space=pltpu.VMEM)],
        scratch_shapes=[
            vmem((4, n * part, tokens), BF),
            vmem((2, tokens, d), BF),
            vmem((tokens, d), jnp.float32),
            vmem((wide, d), BF),
            vmem((d, 2 * wide), BF),
            vmem((2, 512, wide), jnp.float32),
            vmem((2, 512, wide), jnp.float32),
            vmem((2, 256, d), BF),
            vmem((SUM_CHIP + 1, *block), jnp.float32),
            vmem((SUM_NEAR + 1, 2, *block), jnp.float32),
            vmem((SUM_ALL + 1, *block), jnp.float32),
            vmem((2, n // 2, *block), BF),
            vmem((2, n // 2, *block), BF),
            vmem((FAR, *block), BF),
            vmem((FAR, *block), BF),
            vmem((NEAR, 2, *block), BF),
            vmem((NEAR, 2, *block), BF),
            vmem((2, *block), BF),
            vmem((8, wide), jnp.float32),
            vmem((n, 8, 128), jnp.float32),
            dma((4,)),
            dma(()),
            dma((2,)),
            dma((2, 2)),
            dma((2,)),
            dma((2, 2)),
            dma((2,)),
            dma((2,)),
            dma((FAR, 2)),
            dma((FAR, 2)),
            dma((NEAR, 2)),
            dma((NEAR, 2)),
            pltpu.SemaphoreType.REGULAR,
            pltpu.SemaphoreType.REGULAR((2,)),
            pltpu.SemaphoreType.REGULAR((2,)),
            dma((2,)),
        ],
        compiler_params=pltpu.CompilerParams(collective_id=1, has_side_effects=True, vmem_limit_bytes=63 * 2**20),
        cost_estimate=pl.CostEstimate(flops=20 * tokens * d * ff, bytes_accessed=4 * layers * tokens * ff * 4, transcendentals=0),
    )(dy, h, a_t, hid_t, gate, up, *whole)


def solution(mesh):
    n = mesh.shape["dp"]

    def step(x, dy, *arrays):
        weights, m, v = (arrays[i : i + 3] for i in (0, 3, 6))
        gate, up, hid_t, a_t, h, *whole = forward(x[0], *weights, n)
        *gradients, factor = backward(dy[0], h, a_t, hid_t, gate, up, whole, n)
        factor = factor[0, 0]
        new = [adamw(w.astype(jnp.float32), m, v, g.astype(jnp.float32) * factor) for w, m, v, g in zip(weights, m, v, gradients, strict=True)]
        return tuple(one[which] for which in range(3) for one in new)

    states, cut = P(("rep", "dp"), None, None), P(None, "dp", None)
    return jax.shard_map(
        step,
        mesh=mesh,
        in_specs=(states, states) + (cut,) * 9,
        out_specs=(P("rep", "dp", None),) * 9,
        check_vma=False,
    )
```
